768 devices in a mesh: gx: 12 (over z), gy: 64 (over y, x, core).
Axes of the slice: x: 4, y: 8, z: 12, core: 2. Of those that a mesh axis runs over, the one named last changes fastest.
Arguments:
- rock_class: int32 [96, 1024, 128], P('gx', 'gy'), may hold values from 0 to 15
- well_mask: int32 [96, 1024, 128], P('gx', 'gy'), may hold values 0 or 1
- perm_table: float32 [16], replicated, may hold values from 0.01 to 1
- poro_table: float32 [16], replicated, may hold values from 0.05 to 0.35
- accum: float32 [3, 3, 96, 1024, 128], P(None, None, 'gx', 'gy'), may hold values from -0.6 to 2, as said below
- mobility: float32 [3, 96, 1024, 128], P(None, 'gx', 'gy'), may hold values from 0.2 to 2
- right_side: float32 [3, 96, 1024, 128], P(None, 'gx', 'gy'), may hold values from -30 to 30
Outputs:
- pressure: float32 [96, 1024, 128], P('gx', 'gy')
- correction: float32 [3, 96, 1024, 128], P(None, 'gx', 'gy')
The draws below stay inside these ranges and needn't reach their ends.
Inputs may be any that keep to these rules, and one draw needn't show every extreme that they name: `accum`: in each cell's 3 x 3 block the diagonal entries are positive and every off-diagonal entry is at most 0.3 times its row's diagonal entry in magnitude.
All inputs are finite; a program needn't handle non-finite values. No bound on the sum of `well_mask` on one device may be relied on, other than what follows from the above.
Results may differ from the reference program's by a relative error of at most 0.0001.
Values sent between devices are 32-bit elements; how exact they have to be, the bound alone decides.
A program may use at most 32 MiB of HBM per device.

```python
import math
import jax
import jax.numpy as jnp

CLASSES = 16
ITERS = 3
SWEEPS = 2
NX = 96
NY = 1024
NZ = 128


def draw_accum(key, part):
    subkeys = jax.random.split(jax.random.fold_in(key, 11), 2)
    diagonal = jnp.exp(jax.random.uniform(subkeys[0], (3, NX, NY, NZ), jnp.float32, jnp.log(0.2), jnp.log(2.0)))
    ratios = jax.random.uniform(subkeys[1], (3, 3, NX, NY, NZ), jnp.float32, -0.3, 0.3)
    identity = jnp.eye(3, dtype=jnp.float32)[:, :, None, None, None]
    return identity * diagonal[:, None] + (1.0 - identity) * ratios * diagonal[:, None]


def draw_right_side(key, part):
    subkey = jax.random.fold_in(key, 23)
    first_rise = (jnp.arange(NX, dtype=jnp.float32) / NX)[:, None, None]
    second_rise = (jnp.arange(NY, dtype=jnp.float32) / NY)[None, :, None]
    scaling = 0.4 * (1.0 + 2.0 * first_rise) * (1.0 + 2.0 * second_rise)
    noise = jnp.clip(jax.random.normal(subkey, (3, NX, NY, NZ), jnp.float32), -6.0, 6.0)
    return noise * scaling


def plant(values, rng, least, top_value):
    extent = values.shape
    place = [jax.random.randint(jax.random.fold_in(rng, axis), (), 0, extent[axis]) for axis in range(len(extent))]
    values = values.at[tuple(place)].set(least)
    longest = extent.index(max(extent))
    place[longest] = (place[longest] + 1) % extent[longest]
    return values.at[tuple(place)].set(top_value)


def levels(key, dims, shards, low, high):
    loudness, own = 1.0, jax.random.fold_in(key, 6)
    for dim, blocks in shards:
        heights = jnp.exp(jax.random.uniform(jax.random.fold_in(own, dim), (blocks,), jnp.float32, low / len(shards), high / len(shards)))
        loudness = loudness * jnp.repeat(heights, dims[dim] // blocks).reshape([-1 if axis == dim else 1 for axis in range(len(dims))])
    return loudness


def setup_inputs(seed: int = 0) -> dict:
    streams_of = jax.random.split(jax.random.key(seed), 8)
    return {
        "rock_class": plant(jax.random.randint(streams_of[0], (NX, NY, NZ), 0, CLASSES), jax.random.fold_in(streams_of[0], 1), 0, CLASSES - 1).astype(jnp.int32),
        "well_mask": plant((jax.random.randint(streams_of[1], (NX, NY, NZ), 0, 16) < 1).astype(jnp.int32), jax.random.fold_in(streams_of[1], 1), 0, 1),
        "perm_table": jnp.clip(jnp.exp(jax.random.uniform(streams_of[2], (CLASSES,), jnp.float32, math.log(0.01), math.log(1.0))), 0.01, 1.0),
        "poro_table": jnp.clip(jax.random.uniform(streams_of[3], (CLASSES,), jnp.float32, 0.05, 0.35), 0.05, 0.35),
        "accum": draw_accum(jax.random.fold_in(streams_of[7], 71), 0),
        "mobility": jnp.clip(jnp.exp(math.log(2.0) - 2.3025851 * jax.random.uniform(streams_of[5], (3, NX, NY, NZ), jnp.float32) ** levels(streams_of[5], (3, NX, NY, NZ), ((1, 12), (2, 64)), -0.2, 0.2)), 0.2, 2.0),
        "right_side": draw_right_side(jax.random.fold_in(streams_of[7], 71), 0),
    }


FACE_X = 1.0
FACE_Y = 1.0
FACE_Z = 2.0
WELL_FACTOR = 4.0


def harmonic(left_perm, right_perm, left_safe, right_safe):
    return 2.0 * left_perm * right_perm / (left_safe + right_safe)


def couplings(perm_ext, safe_ext, mobility_ext):
    row_perm = perm_ext[:, 1:-1]
    row_safe = safe_ext[:, 1:-1]
    row_mobility = mobility_ext[:, :, 1:-1]
    cross_x = FACE_X * harmonic(row_perm[:-1], row_perm[1:], row_safe[:-1], row_safe[1:]) * 0.5 * (row_mobility[:, :-1] + row_mobility[:, 1:])
    column_perm = perm_ext[1:-1]
    column_safe = safe_ext[1:-1]
    column_mobility = mobility_ext[:, 1:-1]
    cross_y = FACE_Y * harmonic(column_perm[:, :-1], column_perm[:, 1:], column_safe[:, :-1], column_safe[:, 1:]) * 0.5 * (column_mobility[:, :, :-1] + column_mobility[:, :, 1:])
    center_perm = perm_ext[1:-1, 1:-1]
    center_safe = safe_ext[1:-1, 1:-1]
    center_mobility = mobility_ext[:, 1:-1, 1:-1]
    vertical = FACE_Z * harmonic(center_perm[:, :, :-1], center_perm[:, :, 1:], center_safe[:, :, :-1], center_safe[:, :, 1:]) * 0.5 * (center_mobility[..., :-1] + center_mobility[..., 1:])
    closed = jnp.zeros(vertical.shape[:-1] + (1,), jnp.float32)
    cross_z = jnp.concatenate([closed, vertical, closed], axis=-1)
    return cross_x, cross_y, cross_z


def face_flux(coupling, field_ext):
    cross_x, cross_y, cross_z = coupling
    center = field_ext[..., 1:-1, 1:-1, :]
    closed = jnp.zeros_like(center[..., :1])
    lifted = jnp.concatenate([closed, center, closed], axis=-1)
    totals = cross_x[..., 1:, :, :] * (center - field_ext[..., 2:, 1:-1, :])
    totals = totals + cross_x[..., :-1, :, :] * (center - field_ext[..., :-2, 1:-1, :])
    totals = totals + cross_y[..., :, 1:, :] * (center - field_ext[..., 1:-1, 2:, :])
    totals = totals + cross_y[..., :, :-1, :] * (center - field_ext[..., 1:-1, :-2, :])
    totals = totals + cross_z[..., 1:] * (center - lifted[..., 2:])
    totals = totals + cross_z[..., :-1] * (center - lifted[..., :-2])
    return totals


def phase_diagonal(coupling):
    cross_x, cross_y, cross_z = coupling
    totals = cross_x[..., 1:, :, :] + cross_x[..., :-1, :, :]
    totals = totals + cross_y[..., :, 1:, :] + cross_y[..., :, :-1, :]
    return totals + cross_z[..., 1:] + cross_z[..., :-1]


def identity_blocks():
    return jnp.eye(3, dtype=jnp.float32)[:, :, None, None, None]


def invert_blocks(blocks):
    def cofactor(row_index, column_index):
        next_row = (row_index + 1) % 3
        last_row = (row_index + 2) % 3
        next_col = (column_index + 1) % 3
        last_col = (column_index + 2) % 3
        return blocks[next_row, next_col] * blocks[last_row, last_col] - blocks[next_row, last_col] * blocks[last_row, next_col]
    adjugate = jnp.stack([jnp.stack([cofactor(column_index, row_index) for column_index in range(3)]) for row_index in range(3)])
    determinant = jnp.sum(blocks[0] * adjugate[:, 0], axis=0)
    return adjugate / determinant


def jacobian(storage_block, coupling, phase_well, center, field_ext):
    return jnp.sum(storage_block * center[None], axis=1) + face_flux(coupling, field_ext) + phase_well * center


def reference(rock_class, well_mask, perm_table, poro_table, accum, mobility, right_side):
    permeability = perm_table[rock_class]
    porosity = poro_table[rock_class]
    storage_block = porosity * accum
    well_term = WELL_FACTOR * permeability * well_mask.astype(jnp.float32)
    phase_well = well_term * mobility
    padding = ((1, 1), (1, 1), (0, 0))
    perm_ext = jnp.pad(permeability, padding)
    mobility_ext = jnp.pad(mobility, ((0, 0),) + padding)
    coupling = couplings(perm_ext, perm_ext, mobility_ext)
    summed = tuple(jnp.sum(member, axis=0) for member in coupling)
    storage = jnp.sum(storage_block, axis=(0, 1)) + well_term * jnp.sum(mobility, axis=0)

    def pressure_operator(pressure_field):
        return storage * pressure_field + face_flux(summed, jnp.pad(pressure_field, padding))

    source = jnp.sum(right_side, axis=0)
    solution = jnp.zeros_like(source)
    residual = source
    direction = source
    norm_now = jnp.sum(residual * residual)
    for iteration in range(ITERS):
        images = pressure_operator(direction)
        step_size = norm_now / jnp.sum(direction * images)
        solution = solution + step_size * direction
        residual = residual - step_size * images
        norm_next = jnp.sum(residual * residual)
        direction = residual + (norm_next / norm_now) * direction
        norm_now = norm_next
    pressure = solution
    inverse = invert_blocks(storage_block + identity_blocks() * (phase_diagonal(coupling) + phase_well))
    correction = jnp.broadcast_to(pressure[None], (3,) + pressure.shape)
    for sweep_index in range(SWEEPS):
        defect = right_side - jacobian(storage_block, coupling, phase_well, correction, jnp.pad(correction, ((0, 0),) + padding))
        correction = correction + jnp.sum(inverse * defect[None], axis=1)
    return pressure, correction
```

```python
import functools

import jax
import jax.numpy as jnp
from jax import lax
from jax.experimental import pallas as pl
from jax.experimental.pallas import tpu as pltpu
from jax.sharding import PartitionSpec as P

F32 = jnp.float32
NGX, NGY, CORES = 12, 64, 2
NX, NY, NZ = 8, 16, 128
HALO = 3
EX = NX + 2 * HALO
EY = 40
Y0 = 12
Y1 = Y0 + NY
B0, B1 = 8, 32
FACE_Z = 2.0
WELL_FACTOR = 4.0
N1 = NGX * CORES
N2 = NGY // CORES
TINY = 1e-30
SIDES = ((-1, 0), (1, 0), (0, -1), (0, 1))
CORNERS = ((-1, -1), (-1, 1), (1, -1), (1, 1))


def lookup(classes, table):
    values = [table[i] for i in range(16)]
    for bit in range(4):
        odd = (classes & (1 << bit)) != 0
        values = [
            jnp.where(odd, values[2 * j + 1], values[2 * j]) for j in range(len(values) // 2)
        ]
    return values[0]


def harmonic(a, b):
    return a * b / jnp.maximum(a + b, TINY)


def up(v):
    return pltpu.roll(v, NZ - 1, v.ndim - 1)


def down(v):
    return pltpu.roll(v, 1, v.ndim - 1)


def span(step, depth, start, length):
    if step == 0:
        return (start, length), (start, length)
    if step < 0:
        return (start, depth), (start + length, depth)
    return (start + length - depth, depth), (start - depth, depth)


def kernel(
    rock_h, well_h, perm_s, poro_s, accum_h, mobility_h, right_h,
    pressure_o, correction_o,
    rock, well, accum, right, mob,
    ext, v1, v2, cx, cy, cz, hx, hy, hz,
    poro_v, wterm, coef, binv, ys, zs,
    row1, row2, got1, got2,
    in_sem, main_send, main_recv, mob_send, mob_recv, ys_send, ys_recv, s1_send, s1_recv, s2_send, s2_recv,
):
    gx = lax.axis_index("gx")
    gy = lax.axis_index("gy")
    core = lax.rem(gy, CORES)
    plane = gy // CORES
    rank1 = gx * CORES + core

    def exists(step):
        ok = None
        for s, at, n in ((step[0], gx, NGX), (step[1], gy, NGY)):
            if s:
                this = at > 0 if s < 0 else at < n - 1
                ok = this if ok is None else jnp.logical_and(ok, this)
        return ok

    def on_sides(steps, action):
        for index, step in enumerate(steps):
            pl.when(exists(step))(functools.partial(action, index, step))

    def partner1(offset):
        other = lax.rem(rank1 + offset, N1)
        return (other // CORES, plane * CORES + lax.rem(other, CORES))

    def partner2(offset):
        return (gx, lax.rem(plane + offset, N2) * CORES + core)

    barrier = pltpu.get_barrier_semaphore()

    def greet(index, step):
        pl.semaphore_signal(barrier, inc=1, device_id=(gx + step[0], gy + step[1]))

    on_sides(SIDES + CORNERS, greet)

    @pl.loop(1, N1)
    def _(offset):
        pl.semaphore_signal(barrier, inc=1, device_id=partner1(offset))

    @pl.loop(1, N2)
    def _(offset):
        pl.semaphore_signal(barrier, inc=1, device_id=partner2(offset))

    loads = [
        pltpu.make_async_copy(s, d, in_sem.at[i])
        for i, (s, d) in enumerate(
            (
                (rock_h, rock),
                (well_h, well),
                (mobility_h, mob.at[:, 1 : NX + 1, Y0:Y1]),
                (right_h, right),
                (accum_h, accum),
            )
        )
    ]
    for copy in loads:
        copy.start()

    def closed(step):
        return jnp.logical_not(exists(step))

    for side, rows in ((-1, slice(0, HALO)), (1, slice(NX + HALO, EX))):

        @pl.when(closed((side, 0)))
        def _(side=side, rows=rows):
            ext[:, rows, B0:B1] = jnp.zeros((4, HALO, B1 - B0, NZ), F32)
            line = 0 if side < 0 else NX + 1
            ys[:, line, Y0:Y1] = jnp.zeros((12, NY, NZ), F32)
            mob[:, line, Y0:Y1] = jnp.zeros((3, NY, NZ), F32)

    for side, cols in ((-1, slice(8, Y0)), (1, slice(Y1, Y1 + 4))):

        @pl.when(closed((0, side)))
        def _(side=side, cols=cols):
            @pl.loop(0, EX)
            def _(i):
                ext[:, i, cols] = jnp.zeros((4, 4, NZ), F32)

            @pl.loop(0, NX + 2)
            def _(i):
                ys[:, i, cols] = jnp.zeros((12, 4, NZ), F32)
                mob[:, i, cols] = jnp.zeros((3, 4, NZ), F32)

    for copy in loads:
        copy.wait()

    @pl.loop(0, NX)
    def _(i):
        classes = rock[i]
        perm = lookup(classes, perm_s)
        poro = lookup(classes, poro_s)
        total = mob[0, i + 1, Y0:Y1] + mob[1, i + 1, Y0:Y1] + mob[2, i + 1, Y0:Y1]
        term = WELL_FACTOR * perm * well[i].astype(F32)
        stored = accum[0, 0, i]
        for p in range(3):
            for q in range(3):
                if p or q:
                    stored = stored + accum[p, q, i]
        poro_v[i] = poro
        wterm[i] = term
        ext[0, i + HALO, Y0:Y1] = right[0, i] + right[1, i] + right[2, i]
        ext[1, i + HALO, Y0:Y1] = perm
        ext[2, i + HALO, Y0:Y1] = total
        ext[3, i + HALO, Y0:Y1] = poro * stored + term * total

    pl.semaphore_wait(
        barrier,
        N1 - 1 + N2 - 1 + sum(exists(s).astype(jnp.int32) for s in SIDES + CORNERS),
    )

    def halo_copy(ref, steps, send, recv, depths, first_row, index, step, slot):
        (xs, xn), (xd, _) = span(step[0], depths[index], first_row, NX)
        (ysrc, yn), (yd, _) = span(step[1], depths[index], Y0, NY)
        return pltpu.make_async_remote_copy(
            ref.at[:, xs : xs + xn, ysrc : ysrc + yn],
            ref.at[:, xd : xd + xn, yd : yd + yn],
            send.at[index],
            recv.at[slot],
            device_id=(gx + step[0], gy + step[1]),
        )

    def exchange(ref, steps, send, recv, depths, first_row):
        make = functools.partial(halo_copy, ref, steps, send, recv, depths, first_row)

        def start(index, step):
            make(index, step, steps.index((-step[0], -step[1]))).start()

        def arrived(index, step):
            make(index, step, index).wait_recv()

        def sent(index, step):
            make(index, step, index).wait_send()

        return tuple(functools.partial(on_sides, steps, f) for f in (start, arrived, sent))

    steps8 = SIDES + CORNERS
    main_start, main_arrived, main_sent = exchange(
        ext, steps8, main_send, main_recv, (HALO,) * 4 + (2,) * 4, HALO
    )
    mob_start, mob_arrived, mob_sent = exchange(mob, SIDES, mob_send, mob_recv, (1,) * 4, 1)
    ys_start, ys_arrived, ys_sent = exchange(ys, SIDES, ys_send, ys_recv, (1,) * 4, 1)

    main_start()
    mob_start()
    main_arrived()

    low, mid, high = slice(B0 - 1, B1 - 1), slice(B0, B1), slice(B0 + 1, B1 + 1)
    lane = lax.broadcasted_iota(jnp.int32, (B1 - B0, NZ), 1)

    @pl.loop(0, EX - 1)
    def _(i):
        k = ext[1, i, mid]
        m = ext[2, i, mid]
        face = harmonic(k, ext[1, i + 1, mid])
        hx[i, mid] = face
        cx[i, mid] = face * (m + ext[2, i + 1, mid])
        face = harmonic(k, ext[1, i, high])
        hy[i, mid] = face
        cy[i, mid] = face * (m + ext[2, i, high])
        face = jnp.where(lane == NZ - 1, 0.0, FACE_Z * harmonic(k, up(k)))
        hz[i, mid] = face
        cz[i, mid] = face * (m + up(m))

    def operate(field, i, low, mid, high):
        own = field(i, mid)
        out = ext[3, i, mid] * own
        out = out + cx[i, mid] * (own - field(i + 1, mid))
        out = out + cx[i - 1, mid] * (own - field(i - 1, mid))
        out = out + cy[i, mid] * (own - field(i, high))
        out = out + cy[i, low] * (own - field(i, low))
        flux = cz[i, mid] * (own - up(own))
        return out + flux - down(flux), own

    of_v0 = lambda i, s: ext[0, i, s]
    of_v1 = lambda i, s: v1[i, s]
    of_v2 = lambda i, s: v2[i, s]

    @pl.loop(1, EX - 1)
    def _(i):
        v1[i, mid] = operate(of_v0, i, low, mid, high)[0]

    @pl.loop(2, EX - 2)
    def _(i):
        v2[i, mid] = operate(of_v1, i, low, mid, high)[0]

    own_y = slice(Y0, Y1)

    def moments(i, sums):
        image, second = operate(of_v2, i, slice(Y0 - 1, Y1 - 1), own_y, slice(Y0 + 1, Y1 + 1))
        zeroth, first = ext[0, i, own_y], v1[i, own_y]
        terms = (
            zeroth * zeroth, zeroth * first, first * first,
            first * second, second * second, second * image,
        )
        return tuple(s + t[:8] + t[8:] for s, t in zip(sums, terms))

    sums = lax.fori_loop(HALO, HALO + NX, moments, (jnp.zeros((8, NZ), F32),) * 6)
    sub = lax.broadcasted_iota(jnp.int32, (8, NZ), 0)
    lane8 = lax.broadcasted_iota(jnp.int32, (8, NZ), 1)
    stacked = jnp.zeros((8, NZ), F32)
    for n, s in enumerate(sums):
        stacked = jnp.where(sub == n, jnp.sum(s, axis=0, keepdims=True), stacked)
    per_row = jnp.sum(stacked, axis=1, keepdims=True)
    mine = jnp.sum(jnp.where(sub == lane8, per_row, 0.0), axis=0, keepdims=True)
    row1[0] = mine
    got1[rank1] = mine

    def copy1(offset):
        return pltpu.make_async_remote_copy(
            row1.at[0], got1.at[rank1], s1_send, s1_recv, device_id=partner1(offset)
        )

    def copy2(offset):
        return pltpu.make_async_remote_copy(
            row2.at[0], got2.at[plane], s2_send, s2_recv, device_id=partner2(offset)
        )

    @pl.loop(1, N1)
    def _(offset):
        copy1(offset).start()

    def whole1():
        part = got1.at[pl.ds(0, N1 - 1)]
        return pltpu.make_async_remote_copy(part, part, s1_send, s1_recv, device_id=partner1(1))

    def whole2():
        part = got2.at[pl.ds(0, N2 - 1)]
        return pltpu.make_async_remote_copy(part, part, s2_send, s2_recv, device_id=partner2(1))

    mob_arrived()
    fields = (of_v0, of_v1, of_v2)
    ylow, yhigh = slice(Y0 - 1, Y1 - 1), slice(Y0 + 1, Y1 + 1)

    @pl.loop(0, NX)
    def _(i):
        e, m = i + HALO, i + 1
        faces = (hx[e - 1, own_y], hx[e, own_y], hy[e, ylow], hy[e, own_y], hz[e, own_y])
        diagonal, couple = [], []
        for p in range(3):
            own = mob[p, m, own_y]
            c = [
                faces[0] * (mob[p, m - 1, own_y] + own),
                faces[1] * (mob[p, m + 1, own_y] + own),
                faces[2] * (mob[p, m, ylow] + own),
                faces[3] * (mob[p, m, yhigh] + own),
            ]
            vertical = faces[4] * (own + up(own))
            c += [down(vertical), vertical]
            for n in range(6):
                coef[p, n, i] = c[n]
            couple.append(c)
            diagonal.append(c[0] + c[1] + c[2] + c[3] + c[4] + c[5] + wterm[i] * own)
        poro = poro_v[i]
        b = [[poro * accum[p, q, i] for q in range(3)] for p in range(3)]
        for p in range(3):
            b[p][p] = b[p][p] + diagonal[p]
        adj = [[None] * 3 for _ in range(3)]
        for p in range(3):
            for q in range(3):
                r1, r2, c1, c2 = (q + 1) % 3, (q + 2) % 3, (p + 1) % 3, (p + 2) % 3
                adj[p][q] = b[r1][c1] * b[r2][c2] - b[r1][c2] * b[r2][c1]
        inverse = 1.0 / (b[0][0] * adj[0][0] + b[0][1] * adj[1][0] + b[0][2] * adj[2][0])
        inv = [[adj[p][q] * inverse for q in range(3)] for p in range(3)]
        for p in range(3):
            for q in range(3):
                binv[3 * p + q, i] = inv[p][q]

        def solve(side):
            return [inv[p][0] * side[0] + inv[p][1] * side[1] + inv[p][2] * side[2] for p in range(3)]

        first = solve([right[p, i] for p in range(3)])
        for p in range(3):
            ys[p, m, own_y] = first[p]
        for n, field in enumerate(fields):
            own = field(e, own_y)
            near = (
                field(e - 1, own_y), field(e + 1, own_y), field(e, ylow), field(e, yhigh),
                down(own), up(own),
            )
            side = []
            for p in range(3):
                t = couple[p][0] * near[0]
                for d in range(1, 6):
                    t = t + couple[p][d] * near[d]
                side.append(t)
            result = solve(side)
            for p in range(3):
                ys[3 * n + 3 + p, m, own_y] = result[p]

    ys_start()

    whole1().wait_recv()
    total = got1[0]
    for n in range(1, N1):
        total = total + got1[n]
    row2[0] = total
    got2[plane] = total

    @pl.loop(1, N2)
    def _(offset):
        copy2(offset).start()

    ys_arrived()

    @pl.loop(0, NX)
    def _(i):
        m = i + 1
        for n in range(4):
            side = []
            for p in range(3):
                f = 3 * n + p
                own = ys[f, m, own_y]
                near = (
                    ys[f, m - 1, own_y], ys[f, m + 1, own_y], ys[f, m, ylow], ys[f, m, yhigh],
                    down(own), up(own),
                )
                t = coef[p, 0, i] * near[0]
                for d in range(1, 6):
                    t = t + coef[p, d, i] * near[d]
                side.append(t + right[p, i] if n == 0 else t)
            for p in range(3):
                zs[3 * n + p, i] = (
                    binv[3 * p, i] * side[0] + binv[3 * p + 1, i] * side[1] + binv[3 * p + 2, i] * side[2]
                )

    whole2().wait_recv()
    total = got2[0]
    for n in range(1, N2):
        total = total + got2[n]
    nu = [jnp.broadcast_to(total[:, n : n + 1], (1, NZ)) for n in range(6)]

    def guarded(pivot, scale):
        good = pivot > 1e-7 * scale
        return jnp.where(good, 1.0 / jnp.where(good, pivot, 1.0), 0.0)

    r0 = guarded(nu[1], 0.0)
    l10 = nu[2] * r0
    l20 = nu[3] * r0
    d1 = nu[3] - l10 * nu[2]
    t21 = nu[4] - l20 * nu[2]
    r1 = guarded(d1, nu[3])
    l21 = t21 * r1
    d2 = nu[5] - l20 * nu[3] - l21 * t21
    r2 = guarded(d2, nu[5])
    y1 = nu[1] - l10 * nu[0]
    y2 = nu[2] - l20 * nu[0] - l21 * y1
    a2 = y2 * r2
    a1 = y1 * r1 - l21 * a2
    a0 = nu[0] * r0 - l10 * a1 - l20 * a2
    a0, a1, a2 = (jnp.broadcast_to(a, (NY, NZ)) for a in (a0, a1, a2))

    @pl.loop(0, NX)
    def _(i):
        e = i + HALO
        pressure_o[i] = a0 * ext[0, e, own_y] + a1 * v1[e, own_y] + a2 * v2[e, own_y]
        for p in range(3):
            correction_o[p, i] = zs[p, i] + a0 * zs[3 + p, i] + a1 * zs[6 + p, i] + a2 * zs[9 + p, i]

    main_sent()
    mob_sent()
    ys_sent()
    whole1().wait_send()
    whole2().wait_send()


def shards(rock_class, well_mask, perm_table, poro_table, accum, mobility, right_side):
    any_spec = pl.BlockSpec(memory_space=pl.ANY)
    smem = pl.BlockSpec(memory_space=pltpu.SMEM)
    vmem = pl.BlockSpec(memory_space=pltpu.VMEM)
    field = (NX, NY, NZ)
    dma = pltpu.SemaphoreType.DMA
    return tuple(
        pl.pallas_call(
            kernel,
            name="cpr",
            out_shape=(
                jax.ShapeDtypeStruct(field, F32),
                jax.ShapeDtypeStruct((3,) + field, F32),
            ),
            in_specs=[any_spec, any_spec, smem, smem, any_spec, any_spec, any_spec],
            out_specs=(vmem, vmem),
            scratch_shapes=[
                pltpu.VMEM(field, jnp.int32),
                pltpu.VMEM(field, jnp.int32),
                pltpu.VMEM((3, 3) + field, F32),
                pltpu.VMEM((3,) + field, F32),
                pltpu.VMEM((3, NX + 2, EY, NZ), F32),
                pltpu.VMEM((4, EX, EY, NZ), F32),
            ]
            + [pltpu.VMEM((EX, EY, NZ), F32)] * 8
            + [
                pltpu.VMEM(field, F32),
                pltpu.VMEM(field, F32),
                pltpu.VMEM((3, 6) + field, F32),
                pltpu.VMEM((9,) + field, F32),
                pltpu.VMEM((12, NX + 2, EY, NZ), F32),
                pltpu.VMEM((12,) + field, F32),
                pltpu.VMEM((1, 1, NZ), F32),
                pltpu.VMEM((1, 1, NZ), F32),
                pltpu.VMEM((N1, 1, NZ), F32),
                pltpu.VMEM((N2, 1, NZ), F32),
                dma((5,)),
                dma((8,)), dma((8,)), dma((4,)), dma((4,)), dma((4,)), dma((4,)),
                dma, dma, dma, dma,
            ],
            compiler_params=pltpu.CompilerParams(collective_id=0, has_side_effects=True),
        )(rock_class, well_mask, perm_table, poro_table, accum, mobility, right_side)
    )


def solution(mesh):
    in_specs = (
        P("gx", "gy", None),
        P("gx", "gy", None),
        P(),
        P(),
        P(None, None, "gx", "gy", None),
        P(None, "gx", "gy", None),
        P(None, "gx", "gy", None),
    )
    out_specs = (P("gx", "gy", None), P(None, "gx", "gy", None))
    return jax.shard_map(shards, mesh=mesh, in_specs=in_specs, out_specs=out_specs, check_vma=False)
```
